32 devices in a mesh: grp: 2 (over y), lat: 16 (over z, x, core).
Axes of the slice: x: 2, y: 2, z: 4, core: 2. Of those that a mesh axis runs over, the one named last changes fastest.
Arguments:
- air_field: bfloat16 [96, 384, 1440], P(('grp', 'lat')), parts along dimension 0, may hold values from -6 to 6
- marine_field: bfloat16 [96, 200, 1440], P(('grp', 'lat')), parts along dimension 0, may hold values from -6 to 6
- water_indicator: int32 [48, 1440], P('lat'), may hold values from 0 to 1, as said below
- seam_mirror_meridian: int32 [1440], replicated, may hold values from 0 to 1439, as said below
- driving_air_latitude_index: int32 [48], P('lat'), may hold values from 0 to 46, as said below
- marine_latitude_beneath: int32 [48], P('lat'), may hold values from 0 to 47, as said below
- air_rescale_factor: float32 [384], replicated, may hold values from 0.5 to 1.5
- spectral_order_damping: float32 [48, 384], replicated, may hold values from -12 to 12
- feature_blend_matrix: bfloat16 [384, 384], replicated, may hold values from -0.3125 to 0.3125
- boundary_exchange_matrix: bfloat16 [8, 384], replicated, may hold values from -0.3125 to 0.3125
- skin_heat_response: float32 [384], replicated, may hold values from -6 to 6
- driving_feature_matrix: bfloat16 [200, 8], replicated, may hold values from -2 to 2
- planar_stencil_coefficients: float32 [9, 200], replicated, may hold values from -2 to 2
- marine_rescale_factor: float32 [200], replicated, may hold values from 0.5 to 1.5
- marine_expand_matrix: bfloat16 [800, 200], replicated, may hold values from -0.4375 to 0.4375
- marine_contract_matrix: bfloat16 [200, 800], replicated, may hold values from -0.21875 to 0.21875
Outputs:
- atmosphere_next: bfloat16 [96, 384, 1440], P(('grp', 'lat')), parts along dimension 0
- marine_field_advanced: bfloat16 [96, 200, 1440], P(('grp', 'lat')), parts along dimension 0
The draws below stay inside these ranges and needn't reach their ends.
There are 2 independent parts, one for each index of `grp`. The reference program is written for one: setup_inputs(seed, part) draws one part's arguments, and reference() takes and returns one part's arrays. A program takes and returns all parts, laid end to end along the dimension named above; an argument that names none is the same for every part. Nothing has to cross between parts.
Inputs may be any that keep to these rules, and one draw needn't show every extreme that they name: `water_indicator`: among the rows of one index of lat at most 3240 cells are wet, and exactly 3240 on some index. seam_mirror_meridian[i] = (2 s - 1 - i) mod 1440 for one seam s, so it is its own inverse. Rows driving_air_latitude_index[r] and driving_air_latitude_index[r] + 1 are held by the index of lat that holds row r or by the index before it. Row marine_latitude_beneath[j] is held by the index of lat that holds row j or by the index after it.
All inputs are finite; a program needn't handle non-finite values.
Results may differ from the reference program's by a relative error of at most 0.0059.
Values may be sent and summed in bfloat16 or wider, within the bound.
A program may use at most 128 MiB of HBM per device.

```python
import math
import jax
import jax.numpy as jnp
from jax import lax

ROW_DEV = 3
NLON = 1440
AIR_FEATURES = 384
MMAX = 384
F = 8
OC = 200
EXP = 800
NLAT = 48
WET_DEV = 3240


def permute_cells(random_key):
    return jax.random.permutation(random_key, ROW_DEV * NLON)


def draw_water_indicator(key, part):
    band_count = NLAT // ROW_DEV
    key_count, key_full, key_order = jax.random.split(key, 3)
    counts = jax.random.randint(key_count, (band_count,), WET_DEV // 4, WET_DEV + 1)
    fullest = jax.random.randint(key_full, (), 0, band_count)
    counts = jnp.where(jnp.arange(band_count) == fullest, WET_DEV, counts)
    orders = jax.vmap(permute_cells)(jax.random.split(key_order, band_count))
    wet_cells = (orders < counts[:, None]).astype(jnp.int32)
    return wet_cells.reshape(NLAT, NLON)


def draw_seam_mirror_meridian(key, part):
    seam_index = jax.random.randint(key, (), 0, NLON)
    longitude = jnp.arange(NLON, dtype=jnp.int32)
    return ((2 * seam_index - 1 - longitude) % NLON).astype(jnp.int32)


def draw_driving_air_latitude_index(key, part):
    row_index = jnp.arange(NLAT, dtype=jnp.int32)
    owner_band = row_index // ROW_DEV
    lowest = jnp.maximum(owner_band * ROW_DEV - ROW_DEV, 0)
    highest = owner_band * ROW_DEV + ROW_DEV - 2
    return jax.random.randint(key, (NLAT,), lowest, highest + 1).astype(jnp.int32)


def draw_marine_latitude_beneath(key, part):
    row_index = jnp.arange(NLAT, dtype=jnp.int32)
    owner_band = row_index // ROW_DEV
    lowest = owner_band * ROW_DEV
    highest = jnp.minimum(owner_band * ROW_DEV + 2 * ROW_DEV - 1, NLAT - 1)
    return jax.random.randint(key, (NLAT,), lowest, highest + 1).astype(jnp.int32)


def shard_levels(stream_key, dims, pieces, smallest, largest):
    def one(axis_at, shards_of):
        heights = jax.random.uniform(jax.random.fold_in(jax.random.fold_in(stream_key, 6), axis_at), (shards_of,), jnp.float32, smallest / len(pieces), largest / len(pieces))
        return jnp.repeat(jnp.exp(heights), dims[axis_at] // shards_of).reshape((-1,) + (1,) * (len(dims) - axis_at - 1))

    level = one(*pieces[0])
    for cut in pieces[1:]:
        level = level * one(*cut)
    return level


def scatter_about(key, shape, scale, bound, shards=(), kind=jnp.bfloat16):
    drawn = scale * jax.random.normal(key, shape, jnp.float32)
    if shards:
        drawn = drawn * shard_levels(key, shape, shards, -0.22, 0.18)
    return jnp.clip(drawn, -bound, bound).astype(kind)


def setup_inputs(seed: int = 0, part: int = 0) -> dict:
    arg_keys = jax.random.split(jax.random.key(seed), 17)
    own_keys = jax.random.split(jax.random.fold_in(arg_keys[16], part), 17)
    air_field = scatter_about(own_keys[0], (NLAT, AIR_FEATURES, NLON), 1.0, 6.0, ((0, 16),))
    marine_field = scatter_about(own_keys[1], (NLAT, OC, NLON), 1.0, 6.0, ((0, 16),))
    water_indicator = draw_water_indicator(jax.random.fold_in(arg_keys[16], 71), part)
    seam_mirror_meridian = draw_seam_mirror_meridian(jax.random.fold_in(arg_keys[16], 71), part)
    driving_air_latitude_index = draw_driving_air_latitude_index(jax.random.fold_in(arg_keys[16], 71), part)
    marine_latitude_beneath = draw_marine_latitude_beneath(jax.random.fold_in(arg_keys[16], 71), part)
    air_rescale_factor = jnp.clip(1.0 + 0.1 * jax.random.normal(arg_keys[6], (AIR_FEATURES,), jnp.float32), 0.5, 1.5)
    spectral_order_damping = scatter_about(arg_keys[7], (NLAT, AIR_FEATURES), 2.0, 12.0, (), jnp.float32)
    feature_blend_matrix = scatter_about(arg_keys[8], (AIR_FEATURES, AIR_FEATURES), AIR_FEATURES ** -0.5, 0.3125)
    boundary_exchange_matrix = scatter_about(arg_keys[9], (F, AIR_FEATURES), AIR_FEATURES ** -0.5, 0.3125)
    skin_heat_response = scatter_about(arg_keys[10], (AIR_FEATURES,), 1.0, 6.0, (), jnp.float32)
    driving_feature_matrix = scatter_about(arg_keys[11], (OC, F), F ** -0.5, 2.0)
    planar_stencil_coefficients = scatter_about(arg_keys[12], (9, OC), 9 ** -0.5, 2.0, (), jnp.float32)
    marine_rescale_factor = jnp.clip(1.0 + 0.1 * jax.random.normal(arg_keys[13], (OC,), jnp.float32), 0.5, 1.5)
    marine_expand_matrix = scatter_about(arg_keys[14], (EXP, OC), OC ** -0.5, 0.4375)
    marine_contract_matrix = scatter_about(arg_keys[15], (OC, EXP), EXP ** -0.5, 0.21875)
    return {"air_field": air_field, "marine_field": marine_field, "water_indicator": water_indicator, "seam_mirror_meridian": seam_mirror_meridian, "driving_air_latitude_index": driving_air_latitude_index, "marine_latitude_beneath": marine_latitude_beneath, "air_rescale_factor": air_rescale_factor, "spectral_order_damping": spectral_order_damping, "feature_blend_matrix": feature_blend_matrix, "boundary_exchange_matrix": boundary_exchange_matrix, "skin_heat_response": skin_heat_response, "driving_feature_matrix": driving_feature_matrix, "planar_stencil_coefficients": planar_stencil_coefficients, "marine_rescale_factor": marine_rescale_factor, "marine_expand_matrix": marine_expand_matrix, "marine_contract_matrix": marine_contract_matrix}


EPSILON = 1e-05
GELU_SCALE = 0.7978845608028654

def tanh_gelu(values):
    return 0.5 * values * (1.0 + jnp.tanh(GELU_SCALE * (values + 0.044715 * values * values * values)))

def channel_norm(values, gain):
    average = lax.optimization_barrier(jnp.mean(values, axis=-2, keepdims=True))
    centered = values - average
    variance = lax.optimization_barrier(jnp.mean(centered * centered, axis=-2, keepdims=True))
    return centered * lax.rsqrt(variance + EPSILON) * gain[:, None]

def fourier_table(lon_count, mode_count):
    longitude = jnp.arange(lon_count, dtype=jnp.int32)
    harmonic = jnp.arange(mode_count, dtype=jnp.int32)
    phase_index = longitude[:, None] * harmonic[None, :] % lon_count
    angles = 2.0 * math.pi / lon_count * phase_index.astype(jnp.float32)
    scaled = jnp.concatenate([jnp.cos(angles), jnp.sin(angles)], axis=1) / math.sqrt(lon_count)
    return scaled.astype(jnp.bfloat16)

def latitude_table(row_count):
    row_index = jnp.arange(row_count, dtype=jnp.int32)
    phase_index = (2 * row_index[:, None] + 1) * row_index[None, :] % (4 * row_count)
    angles = math.pi / (2.0 * row_count) * phase_index.astype(jnp.float32)
    return (jnp.cos(angles) * math.sqrt(2.0 / row_count)).astype(jnp.bfloat16)

def depth_conv(extended, planar_stencil_coefficients, row_count):
    summed = jnp.zeros((row_count,) + extended.shape[1:], jnp.float32)
    for vertical in range(3):
        row_band = extended[vertical:vertical + row_count].astype(jnp.float32)
        for horizontal in range(3):
            shifted = jnp.roll(row_band, 1 - horizontal, axis=2)
            summed = summed + planar_stencil_coefficients[3 * vertical + horizontal][None, :, None] * shifted
    return summed

def reference(air_field, marine_field, water_indicator, seam_mirror_meridian, driving_air_latitude_index, marine_latitude_beneath, air_rescale_factor, spectral_order_damping, feature_blend_matrix, boundary_exchange_matrix, skin_heat_response, driving_feature_matrix, planar_stencil_coefficients, marine_rescale_factor, marine_expand_matrix, marine_contract_matrix):
    atmos_float = air_field.astype(jnp.float32)
    flux = jnp.einsum('fc,jcl->jfl', boundary_exchange_matrix.astype(jnp.float32), atmos_float).astype(jnp.bfloat16)
    lower_rows = jnp.take(flux, driving_air_latitude_index, axis=0).astype(jnp.float32)
    upper_rows = jnp.take(flux, driving_air_latitude_index + 1, axis=0).astype(jnp.float32)
    forcing = 0.5 * (lower_rows + upper_rows)
    wet_float = water_indicator.astype(jnp.float32)[:, None, :]
    push = jnp.einsum('kf,rfl->rkl', driving_feature_matrix.astype(jnp.float32), forcing, precision=lax.Precision.HIGHEST)
    forced = (marine_field.astype(jnp.float32) + wet_float * push).astype(jnp.bfloat16)
    folded = jnp.take(forced[-1], seam_mirror_meridian, axis=1)
    extended = jnp.concatenate([jnp.zeros_like(forced[:1]), forced, folded[None]], axis=0)
    depth = depth_conv(extended, planar_stencil_coefficients, forced.shape[0])
    ocean_normed = channel_norm(depth, marine_rescale_factor).astype(jnp.bfloat16)

    def ocean_row(inputs):
        normed_row, forced_row, wet_row = inputs
        hidden = tanh_gelu(jnp.dot(marine_expand_matrix, normed_row, preferred_element_type=jnp.float32)).astype(jnp.bfloat16)
        update = jnp.dot(marine_contract_matrix, hidden, preferred_element_type=jnp.float32)
        return ((forced_row.astype(jnp.float32) + update) * wet_row[None, :]).astype(jnp.bfloat16)
    marine_field_advanced = lax.map(ocean_row, (ocean_normed, forced, water_indicator.astype(jnp.float32)))
    skin_heat_aloft = jnp.take(marine_field_advanced[:, 0, :], marine_latitude_beneath, axis=0)
    atm_normed = channel_norm(atmos_float, air_rescale_factor).astype(jnp.bfloat16)
    table = fourier_table(air_field.shape[2], MMAX).astype(jnp.float32)
    coefficients = jnp.einsum('jcl,lm->jcm', atm_normed.astype(jnp.float32), table).astype(jnp.bfloat16)
    lat_table = latitude_table(air_field.shape[0]).astype(jnp.float32)
    spectrum = jnp.einsum('jl,jcm->lcm', lat_table, coefficients.astype(jnp.float32))
    filtered = (spectrum * spectral_order_damping[:, :, None]).astype(jnp.bfloat16)
    returned = jnp.einsum('jl,lcm->jcm', lat_table, filtered.astype(jnp.float32)).astype(jnp.bfloat16)
    grid_values = jnp.einsum('jcm,lm->jcl', returned.astype(jnp.float32), table)
    activation = tanh_gelu(grid_values).astype(jnp.bfloat16)
    mixed = jnp.einsum('dc,jcl->jdl', feature_blend_matrix.astype(jnp.float32), activation.astype(jnp.float32))
    joint_outcome = skin_heat_response[None, :, None] * skin_heat_aloft.astype(jnp.float32)[:, None, :]
    atmosphere_next = (atmos_float + mixed + joint_outcome).astype(jnp.bfloat16)
    return (atmosphere_next, marine_field_advanced)
```

```python
import math

import jax
import jax.numpy as jnp
import numpy as np
from jax import lax
from jax.experimental import pallas as pl
from jax.experimental.pallas import tpu as pltpu
from jax.sharding import PartitionSpec as P

MMAX = 384


EPSILON = 1e-05
GELU_SCALE = 0.7978845608028654
GROUP = 16


def shifted_2(array, axis, by):
    size = lax.axis_size(axis)
    pairs = [(i, i + by) for i in range(size) if 0 <= i + by < size]
    return lax.ppermute(array, axis, pairs)


def halo_rows(array, axis):
    size = lax.axis_size(axis)
    up = [(i, i + 1) for i in range(size - 1)]
    down = [(j, i) for i, j in up]
    before = lax.ppermute(array[-1:], axis, up)
    after = lax.ppermute(array[:1], axis, down)
    return before, after


def tanh_gelu(values):
    return (
        0.5 * values * (1.0 + jnp.tanh(GELU_SCALE * (values + 0.044715 * values * values * values)))
    )


def channel_norm(values, gain):
    average = jnp.mean(values, axis=-2, keepdims=True)
    centered = values - average
    variance = jnp.mean(centered * centered, axis=-2, keepdims=True)
    return centered * lax.rsqrt(variance + EPSILON) * gain[:, None]


def fourier_rows(lon_count, mode_count):
    phase = np.arange(mode_count)[:, None] * np.arange(lon_count)[None, :] % lon_count
    angles = 2.0 * math.pi / lon_count * phase
    table = np.concatenate([np.cos(angles), np.sin(angles)], axis=0) / math.sqrt(lon_count)
    return table.astype(jnp.bfloat16)


def latitude_values(row_count):
    index = np.arange(row_count)
    phase = (2 * index[:, None] + 1) * index[None, :] % (4 * row_count)
    angles = math.pi / (2.0 * row_count) * phase
    return (np.cos(angles) * math.sqrt(2.0 / row_count)).astype(jnp.bfloat16)


def latitude_blocks(bands, rows):
    values = latitude_values(bands * rows).astype(np.float32).reshape(bands, rows, bands * rows)
    same = np.eye(GROUP, dtype=np.float32)
    full = np.einsum("bjl,pq->lpjbq", values, same)
    return full.reshape(bands * rows * GROUP, rows * bands * GROUP).astype(jnp.bfloat16)


def forward_kernel(x_ref, table_ref, gain_ref, exchange_ref, coef_ref, flux_ref):
    raw = x_ref[0]
    flux_ref[0] = lax.dot_general(
        exchange_ref[...], raw, (((1,), (1,)), ((), ())), preferred_element_type=jnp.float32
    ).astype(jnp.bfloat16)
    values = raw.astype(jnp.float32)
    average = jnp.mean(values, axis=-1, keepdims=True)
    centered = values - average
    variance = jnp.mean(centered * centered, axis=-1, keepdims=True)
    normed = (centered * lax.rsqrt(variance + EPSILON) * gain_ref[...]).astype(jnp.bfloat16)
    coef_ref[...] = jnp.dot(
        table_ref[...], normed, preferred_element_type=jnp.float32
    ).astype(jnp.bfloat16)


def forward_transform(air_rows, table, gain, exchange):
    rows, lon_count, channels = air_rows.shape
    modes, fields = table.shape[0], exchange.shape[0]
    return pl.pallas_call(
        forward_kernel,
        grid=(rows,),
        in_specs=[
            pl.BlockSpec((1, lon_count, channels), lambda j: (j, 0, 0)),
            pl.BlockSpec((modes, lon_count), lambda j: (0, 0)),
            pl.BlockSpec((1, channels), lambda j: (0, 0)),
            pl.BlockSpec((fields, channels), lambda j: (0, 0)),
        ],
        out_specs=[
            pl.BlockSpec((modes, channels), lambda j: (0, j)),
            pl.BlockSpec((1, fields, lon_count), lambda j: (j, 0, 0)),
        ],
        out_shape=[
            jax.ShapeDtypeStruct((modes, rows * channels), jnp.bfloat16),
            jax.ShapeDtypeStruct((rows, fields, lon_count), jnp.bfloat16),
        ],
        cost_estimate=pl.CostEstimate(
            flops=2 * rows * lon_count * channels * modes,
            bytes_accessed=2 * (rows * lon_count * channels + modes * (lon_count + rows * channels)),
            transcendentals=0,
        ),
    )(air_rows, table, gain[None, :], exchange)


def filter_kernel(got_ref, blocks_ref, back_ref, damping_ref, out_ref):
    bands, group, lanes = got_ref.shape
    depth = bands * group
    rows = blocks_ref.shape[1] // depth
    channels = lanes // rows
    spectrum = jnp.zeros((blocks_ref.shape[0], channels), jnp.float32)
    for j in range(rows):
        part = got_ref[:, :, j * channels : (j + 1) * channels].reshape(depth, channels)
        spectrum = spectrum + jnp.dot(
            blocks_ref[:, j * depth : (j + 1) * depth], part, preferred_element_type=jnp.float32
        )
    filtered = (spectrum * damping_ref[...]).astype(jnp.bfloat16)
    for j in range(rows):
        back = jnp.dot(
            back_ref[j * depth : (j + 1) * depth, :], filtered, preferred_element_type=jnp.float32
        )
        out_ref[:, :, j * channels : (j + 1) * channels] = back.astype(jnp.bfloat16).reshape(
            bands, group, channels
        )


def latitude_filter(gathered, damping, rows):
    bands, own, lanes = gathered.shape
    channels = lanes // rows
    if own % GROUP or bands > GROUP:
        split = gathered.reshape(bands, own, rows, channels)
        table = jnp.asarray(latitude_values(bands * rows)).reshape(bands, rows, bands * rows)
        spectrum = jnp.einsum("bjl,bqjc->lqc", table, split, preferred_element_type=jnp.float32)
        filtered = (spectrum * damping[:, None, :]).astype(jnp.bfloat16)
        back = jnp.einsum("bjl,lqc->bqjc", table, filtered, preferred_element_type=jnp.float32)
        return back.astype(jnp.bfloat16).reshape(gathered.shape)
    blocks = lax.optimization_barrier(jnp.asarray(latitude_blocks(bands, rows)))
    side = blocks.shape[0]
    damping_rows = jnp.repeat(damping, GROUP, axis=0)
    return pl.pallas_call(
        filter_kernel,
        grid=(own // GROUP,),
        in_specs=[
            pl.BlockSpec((bands, GROUP, lanes), lambda g: (0, g, 0)),
            pl.BlockSpec((side, side), lambda g: (0, 0)),
            pl.BlockSpec((side, side), lambda g: (0, 0)),
            pl.BlockSpec((side, channels), lambda g: (0, 0)),
        ],
        out_specs=pl.BlockSpec((bands, GROUP, lanes), lambda g: (0, g, 0)),
        out_shape=jax.ShapeDtypeStruct(gathered.shape, jnp.bfloat16),
        cost_estimate=pl.CostEstimate(
            flops=4 * side * side * channels * (own // GROUP),
            bytes_accessed=4 * gathered.size + 4 * side * side,
            transcendentals=0,
        ),
    )(gathered, blocks, blocks.T, damping_rows)


def inverse_kernel(back_ref, table_ref, blend_ref, x_ref, sst_ref, skin_ref, out_ref):
    grid_values = jnp.dot(table_ref[...], back_ref[...], preferred_element_type=jnp.float32)
    activation = tanh_gelu(grid_values).astype(jnp.bfloat16)
    mixed = lax.dot_general(
        activation, blend_ref[...], (((1,), (1,)), ((), ())), preferred_element_type=jnp.float32
    )
    skin = skin_ref[...]
    high = skin.astype(jnp.bfloat16).astype(jnp.float32)
    middle = (skin - high).astype(jnp.bfloat16).astype(jnp.float32)
    low = skin - high - middle
    level = lax.broadcasted_iota(jnp.int32, (8, skin.shape[1]), 0)
    pieces = jnp.where(
        level == 0, high, jnp.where(level == 1, middle, jnp.where(level == 2, low, 0.0))
    ).astype(jnp.bfloat16)
    warmth = jnp.broadcast_to(sst_ref[0].astype(jnp.float32), (8, sst_ref.shape[2]))
    joint = lax.dot_general(
        warmth.astype(jnp.bfloat16),
        pieces,
        (((0,), (0,)), ((), ())),
        preferred_element_type=jnp.float32,
    )
    out_ref[0] = (x_ref[0].astype(jnp.float32) + mixed + joint).astype(jnp.bfloat16)


def inverse_transform(returned, table, blend, air_rows, sst, skin):
    rows, lon_count, channels = air_rows.shape
    modes = table.shape[1]
    return pl.pallas_call(
        inverse_kernel,
        grid=(rows,),
        in_specs=[
            pl.BlockSpec((modes, channels), lambda j: (0, j)),
            pl.BlockSpec((lon_count, modes), lambda j: (0, 0)),
            pl.BlockSpec((channels, channels), lambda j: (0, 0)),
            pl.BlockSpec((1, lon_count, channels), lambda j: (j, 0, 0)),
            pl.BlockSpec((1, 1, lon_count), lambda j: (j, 0, 0)),
            pl.BlockSpec((1, channels), lambda j: (0, 0)),
        ],
        out_specs=pl.BlockSpec((1, lon_count, channels), lambda j: (j, 0, 0)),
        out_shape=jax.ShapeDtypeStruct(air_rows.shape, jnp.bfloat16),
        cost_estimate=pl.CostEstimate(
            flops=2 * rows * lon_count * channels * (modes + channels),
            bytes_accessed=4 * rows * lon_count * channels + 2 * modes * (lon_count + channels),
            transcendentals=rows * lon_count * channels,
        ),
    )(returned, table, blend, air_rows, sst[:, None, :], skin[None, :])


def depth_conv(extended, planar_stencil_coefficients, row_count):
    summed = jnp.zeros((row_count,) + extended.shape[1:], jnp.float32)
    for vertical in range(3):
        row_band = extended[vertical : vertical + row_count].astype(jnp.float32)
        for horizontal in range(3):
            shifted = jnp.roll(row_band, 1 - horizontal, axis=2)
            summed = (
                summed
                + planar_stencil_coefficients[3 * vertical + horizontal][None, :, None] * shifted
            )
    return summed


def local(
    air_field,
    marine_field,
    water_indicator,
    seam_mirror_meridian,
    driving_air_latitude_index,
    marine_latitude_beneath,
    air_rescale_factor,
    spectral_order_damping,
    feature_blend_matrix,
    boundary_exchange_matrix,
    skin_heat_response,
    driving_feature_matrix,
    planar_stencil_coefficients,
    marine_rescale_factor,
    marine_expand_matrix,
    marine_contract_matrix,
):
    row_count, channels, lon_count = air_field.shape
    band_count = lax.axis_size("lat")
    band_index = lax.axis_index("lat")
    first_row = band_index * row_count
    air_rows = air_field.transpose(0, 2, 1)
    table = lax.optimization_barrier(jnp.asarray(fourier_rows(lon_count, MMAX)))
    modes = table.shape[0]
    coefficients, flux = forward_transform(
        air_rows, table, air_rescale_factor, boundary_exchange_matrix
    )
    gathered = lax.all_to_all(coefficients, "lat", split_axis=0, concat_axis=0, tiled=True)

    earlier = shifted_2(flux, "lat", 1)
    flux_window = jnp.concatenate([earlier, flux], axis=0)
    offsets = driving_air_latitude_index - (first_row - row_count)
    lower_rows = jnp.take(flux_window, offsets, axis=0)
    upper_rows = jnp.take(flux_window, offsets + 1, axis=0)
    forcing = 0.5 * (lower_rows.astype(jnp.float32) + upper_rows.astype(jnp.float32))
    wet_float = water_indicator.astype(jnp.float32)[:, None, :]
    push = jnp.einsum(
        "kf,rfl->rkl",
        driving_feature_matrix.astype(jnp.float32),
        forcing,
        precision=lax.Precision.HIGHEST,
    )
    forced = (marine_field.astype(jnp.float32) + wet_float * push).astype(jnp.bfloat16)
    before, after = halo_rows(forced, "lat")
    folded = jnp.take(forced[-1], seam_mirror_meridian, axis=1)

    filtered_back = latitude_filter(
        gathered.reshape(band_count, modes // band_count, row_count * channels),
        spectral_order_damping,
        row_count,
    )
    returned = lax.all_to_all(
        filtered_back.reshape(modes, row_count * channels),
        "lat",
        split_axis=0,
        concat_axis=0,
        tiled=True,
    )

    before, after, folded, _ = lax.optimization_barrier(
        (before, after, folded, filtered_back[0, 0, 0])
    )
    top_row = jnp.where(band_index == band_count - 1, folded[None], after)
    extended = jnp.concatenate([before, forced, top_row], axis=0)
    depth = depth_conv(extended, planar_stencil_coefficients, row_count)
    ocean_normed = channel_norm(depth, marine_rescale_factor).astype(jnp.bfloat16)
    hidden = tanh_gelu(
        jnp.einsum(
            "ek,rkl->rel", marine_expand_matrix, ocean_normed, preferred_element_type=jnp.float32
        )
    ).astype(jnp.bfloat16)
    update = jnp.einsum(
        "ke,rel->rkl", marine_contract_matrix, hidden, preferred_element_type=jnp.float32
    )
    marine_field_advanced = ((forced.astype(jnp.float32) + update) * wet_float).astype(jnp.bfloat16)
    skin_heat = marine_field_advanced[:, 0, :]
    following = shifted_2(skin_heat, "lat", -1)
    temp_window = jnp.concatenate([skin_heat, following], axis=0)
    skin_heat_aloft = jnp.take(temp_window, marine_latitude_beneath - first_row, axis=0)

    outcome = inverse_transform(
        returned, table.T, feature_blend_matrix, air_rows, skin_heat_aloft, skin_heat_response
    )
    return (outcome.transpose(0, 2, 1), marine_field_advanced)


def solution(mesh):
    return jax.shard_map(
        local,
        mesh=mesh,
        in_specs=(
            P(("grp", "lat"), None, None),
            P(("grp", "lat"), None, None),
            P("lat", None),
            P(),
            P("lat"),
            P("lat"),
            P(),
            P(),
            P(),
            P(),
            P(),
            P(),
            P(),
            P(),
            P(),
            P(),
        ),
        out_specs=(P(("grp", "lat"), None, None), P(("grp", "lat"), None, None)),
        check_vma=False,
    )
```
